256 devices in a mesh: zero: 32 (over y, x, core), tp: 8 (over z).
Axes of the slice: x: 4, y: 4, z: 8, core: 2. Of those that a mesh axis runs over, the one named last changes fastest.
Arguments:
- weight_gate: bfloat16 [2560, 9728], P('zero', 'tp'), may hold values from -0.125 to 0.125
- low_gate: bfloat16 [2560, 16], P('zero'), may hold values from -0.125 to 0.125
- high_gate: bfloat16 [16, 9728], P(None, 'tp'), may hold values from -1.5 to 1.5
- weight_up: bfloat16 [2560, 9728], P('zero', 'tp'), may hold values from -0.125 to 0.125
- low_up: bfloat16 [2560, 16], P('zero'), may hold values from -0.125 to 0.125
- high_up: bfloat16 [16, 9728], P(None, 'tp'), may hold values from -1.5 to 1.5
- weight_down: bfloat16 [9728, 2560], P('tp', 'zero'), may hold values from -0.0625 to 0.0625
- low_down: bfloat16 [9728, 16], P('tp'), may hold values from -0.0625 to 0.0625
- high_down: bfloat16 [16, 2560], P(None, 'zero'), may hold values from -1.5 to 1.5
- norm_train: float32 [2560], P(('zero', 'tp')), may hold values from 0.25 to 1.75
- norm_step: float32 [2560], P(('zero', 'tp')), may hold values from -0.3 to 0.3
Outputs:
- ready_gate: bfloat16 [2560, 9728], P(None, 'tp')
- ready_up: bfloat16 [2560, 9728], P(None, 'tp')
- ready_down: bfloat16 [9728, 2560], P('tp')
- serve_norm: bfloat16 [2560], replicated
The draws below stay inside these ranges and needn't reach their ends.
All inputs are finite; a program needn't handle non-finite values.
Results may differ from the reference program's by a relative error of at most 0.001.
Values may be sent and summed in bfloat16 or wider, within the bound.
A program may use at most 128 MiB of HBM per device.

```python
import jax
import jax.numpy as jnp

D_MODEL = 2560
D_INNER = 9728
RANK = 16


def shard_levels(own_key, dims, shards, low, top_value):
    def one(dim, parts):
        steps = jax.random.uniform(jax.random.fold_in(jax.random.fold_in(own_key, 6), dim), (parts,), jnp.float32, low / len(shards), top_value / len(shards))
        return jnp.repeat(jnp.exp(steps), dims[dim] // parts).reshape((-1,) + (1,) * (len(dims) - dim - 1))

    loudness = one(*shards[0])
    for cut in shards[1:]:
        loudness = loudness * one(*cut)
    return loudness


def gaussian(stream_key, shape, spread, most, shards=(), kind=jnp.bfloat16):
    array = jax.random.normal(stream_key, shape, jnp.float32) * spread
    if len(shards) > 0:
        array = shard_levels(stream_key, shape, shards, -0.22, 0.18) * array
    return jnp.clip(array, min=-most, max=most).astype(kind)


def setup_inputs(seed: int = 0) -> dict:
    key_of = jax.random.split(jax.random.key(seed), 12)
    return {
        "weight_gate": gaussian(key_of[0], (D_MODEL, D_INNER), D_MODEL ** -0.5, 0.125, ((0, 32), (1, 8))),
        "low_gate": gaussian(key_of[1], (D_MODEL, RANK), D_MODEL ** -0.5, 0.125, ((0, 32),)),
        "high_gate": gaussian(key_of[2], (RANK, D_INNER), RANK ** -0.5, 1.5, ((1, 8),)),
        "weight_up": gaussian(key_of[3], (D_MODEL, D_INNER), D_MODEL ** -0.5, 0.125, ((0, 32), (1, 8))),
        "low_up": gaussian(key_of[4], (D_MODEL, RANK), D_MODEL ** -0.5, 0.125, ((0, 32),)),
        "high_up": gaussian(key_of[5], (RANK, D_INNER), RANK ** -0.5, 1.5, ((1, 8),)),
        "weight_down": gaussian(key_of[6], (D_INNER, D_MODEL), D_INNER ** -0.5, 0.0625, ((0, 8), (1, 32))),
        "low_down": gaussian(key_of[7], (D_INNER, RANK), D_INNER ** -0.5, 0.0625, ((0, 8),)),
        "high_down": gaussian(key_of[8], (RANK, D_MODEL), RANK ** -0.5, 1.5, ((1, 32),)),
        "norm_train": jnp.clip(1.0 + 0.15 * jax.random.normal(key_of[9], (D_MODEL,), jnp.float32), 0.25, 1.75),
        "norm_step": jnp.clip(jax.random.uniform(key_of[10], (D_MODEL,), jnp.float32, -0.3, 0.3) * shard_levels(key_of[10], (D_MODEL,), ((0, 256),), -0.4, 0.0), -0.3, 0.3),
    }


mix_rate = 0.5


def reference(weight_gate, low_gate, high_gate, weight_up, low_up, high_up, weight_down, low_down, high_down, norm_train, norm_step):
    latest_gate = weight_gate.astype(jnp.float32) + mix_rate * jnp.dot(low_gate, high_gate, preferred_element_type=jnp.float32)
    latest_up = weight_up.astype(jnp.float32) + mix_rate * jnp.dot(low_up, high_up, preferred_element_type=jnp.float32)
    latest_down = weight_down.astype(jnp.float32) + mix_rate * jnp.dot(low_down, high_down, preferred_element_type=jnp.float32)
    ready_gate = latest_gate.astype(jnp.bfloat16)
    ready_up = latest_up.astype(jnp.bfloat16)
    ready_down = latest_down.astype(jnp.bfloat16)
    serve_norm = (norm_train + norm_step).astype(jnp.bfloat16)
    return ready_gate, ready_up, ready_down, serve_norm
```

```python
import functools
import heapq

import jax
import jax.numpy as jnp
from jax import lax
from jax.experimental import pallas as pl
from jax.experimental.pallas import tpu as pltpu
from jax.sharding import PartitionSpec as P

MESH = pl.DeviceIdType.MESH
LINKS = ("u+", "u-", "v+", "v-")
SIDE = 4
BLOCK = 80
WIDTH = 1216
RANK = 16
LANE = 128
CHUNKS = {"A0": (0, 7), "A1": (7, 14), "B0": (14, 21), "B1": (21, 29)}
TILES = 29
COLUMNS = TILES * LANE
NORM_LANE = 3 * WIDTH
HALF = LANE // 2

mix_rate = 0.5


def onward(item):
    chunk, ou, ov = item
    first, second = ("u", "v") if chunk[0] == "A" else ("v", "u")
    a, b = (ou, ov) if chunk[0] == "A" else (ov, ou)
    turn = "+" if chunk[1] == "0" else "-"
    far = SIDE - 1 if turn == "+" else 1
    if b == 0:
        out = [first + "+", first + "-"] if a == 0 else [first + turn] if a == far else []
        return out + [second + "+", second + "-"]
    return [second + turn] if b == far else []


def seen_there(item, link):
    chunk, ou, ov = item
    step = SIDE - 1 if link[1] == "+" else 1
    return (chunk, (ou + step) % SIDE, ov) if link[0] == "u" else (chunk, ou, (ov + step) % SIDE)


def depth(item):
    return max((1 + depth(seen_there(item, link)) for link in onward(item)), default=0)


def plan(tile_us=0.44, hop_us=2.5):
    free = dict.fromkeys(LINKS, 0.0)
    ready = {link: [] for link in LINKS}
    sends = {link: [] for link in LINKS}
    arrivals, events, count = [], [], 0
    for chunk in CHUNKS:
        events.append((0.0, count, (chunk, 0, 0)))
        count += 1
    while events:
        now, _, item = heapq.heappop(events)
        if item is not None:
            arrivals.append(item)
            for link in onward(item):
                heapq.heappush(ready[link], (-depth(seen_there(item, link)), count, item))
                count += 1
        if events and events[0][0] <= now + 1e-9:
            continue
        for link in LINKS:
            if free[link] <= now + 1e-9 and ready[link]:
                item = heapq.heappop(ready[link])[2]
                lo, hi = CHUNKS[item[0]]
                free[link] = now + (hi - lo) * tile_us
                sends[link].append(item)
                heapq.heappush(events, (free[link], count, None))
                heapq.heappush(events, (free[link] + hop_us, count + 1, seen_there(item, link)))
                count += 2
    return sends, arrivals


def gather_kernel(
    wg, ag, bg, wu, au, bu, wd, ad, bd, nt, ns, all_ref,
    w, a, b, n, nz, in_sem, recv_sem, norm_send, norm_recv, send_sem, peer_send, peer_recv,
):
    zero, z = lax.axis_index("zero"), lax.axis_index("tp")
    tp = lax.axis_size("tp")
    core, chip = lax.rem(zero, 2), lax.div(zero, 2)
    x, y = lax.rem(chip, SIDE), lax.div(chip, SIDE)

    def at(ou, ov):
        ox = lax.rem(x + (1 - core) * ou - core * ov + SIDE, SIDE)
        oy = lax.rem(y + (1 - core) * ov - core * ou + SIDE, SIDE)
        return (oy * SIDE + ox) * 2 + core

    place = {(ou, ov): at(ou, ov) for ou in range(SIDE) for ov in range(SIDE)}
    target = {"u+": place[1, 0], "u-": place[3, 0], "v+": place[0, 1], "v-": place[0, 3]}
    peer = zero + 1 - 2 * core

    copies = []
    for k, (src, dst) in enumerate(
        [(nt, n.at[0]), (ns, n.at[1])]
        + [
            pair
            for t, refs in enumerate([(wg, ag, bg), (wu, au, bu), (wd, ad, bd)])
            for pair in zip(refs, (w.at[t], a.at[t], b.at[t]))
        ]
    ):
        copy = pltpu.make_async_copy(src, dst, in_sem.at[k])
        copy.start()
        copies.append(copy)

    barrier = pltpu.get_barrier_semaphore()
    others = [lax.rem(z + k, tp) for k in range(1, tp)]
    for other in list(target.values()) + [peer]:
        pl.semaphore_signal(barrier, inc=1, device_id={"zero": other, "tp": z}, device_id_type=MESH)
    for other in others:
        pl.semaphore_signal(barrier, inc=1, device_id={"zero": zero, "tp": other}, device_id_type=MESH)

    copies[0].wait()
    copies[1].wait()
    gain = (n[0] + n[1]).astype(jnp.bfloat16).astype(jnp.float32)
    nz[z] = jnp.concatenate([gain, jnp.zeros((1, LANE - gain.shape[1]), jnp.float32)], axis=1)

    mine = pl.ds(pl.multiple_of(zero * BLOCK, 16), BLOCK)
    latest = []
    for t in range(3):
        for copy in copies[2 + 3 * t : 5 + 3 * t]:
            copy.wait()
        low_high = lax.dot_general(
            a[t], b[t], (((0,), (0,)), ((), ())), preferred_element_type=jnp.float32
        )
        latest.append(w[t].astype(jnp.float32) + mix_rate * low_high)
        if t == 1:
            both = jnp.concatenate(latest, axis=1)
            all_ref[mine, 0 : 2 * WIDTH] = both.astype(jnp.bfloat16)
    cut = WIDTH - HALF
    all_ref[mine, 2 * WIDTH : COLUMNS - LANE] = latest[2][:, :cut].astype(jnp.bfloat16)
    tail = jnp.concatenate([latest[2][:, cut:], jnp.zeros((BLOCK, HALF), jnp.float32)], axis=1)

    pl.semaphore_wait(barrier, len(target) + 1 + len(others))

    norm_copies = []
    for k, other in enumerate(others):
        copy = pltpu.make_async_remote_copy(
            src_ref=nz.at[z], dst_ref=nz.at[z], send_sem=norm_send.at[k], recv_sem=norm_recv.at[k],
            device_id={"zero": zero, "tp": other}, device_id_type=MESH,
        )
        copy.start()
        norm_copies.append(copy)

    def span(item):
        chunk, ou, ov = item
        lo, hi = CHUNKS[chunk]
        rows = pl.ds(pl.multiple_of(place[ou, ov] * BLOCK, 16), BLOCK)
        return all_ref.at[rows, lo * LANE : hi * LANE]

    sends, arrivals = plan()
    number = {item: k for k, item in enumerate(i for i in arrivals if i[1:] != (0, 0))}

    def send(item, link):
        part = span(item)
        pltpu.make_async_remote_copy(
            src_ref=part, dst_ref=part, send_sem=send_sem, recv_sem=recv_sem.at[number[seen_there(item, link)]],
            device_id={"zero": target[link], "tp": z}, device_id_type=MESH,
        ).start()

    def hand_over(item):
        part = span(item)
        pltpu.make_async_remote_copy(
            src_ref=part, dst_ref=part, send_sem=peer_send, recv_sem=peer_recv,
            device_id={"zero": peer, "tp": z}, device_id_type=MESH,
        ).start()

    queue = {link: list(order) for link, order in sends.items()}
    here = set()

    def issue():
        moved = True
        while moved:
            moved = False
            for link in LINKS:
                if queue[link] and queue[link][0] in here:
                    send(queue[link].pop(0), link)
                    moved = True

    here |= {("A0", 0, 0), ("A1", 0, 0), ("B0", 0, 0)}
    issue()

    for copy in norm_copies:
        copy.wait_recv()
    row = lax.broadcasted_iota(jnp.int32, (BLOCK, LANE), 0)
    lane = lax.broadcasted_iota(jnp.int32, (BLOCK, LANE), 1)
    share = BLOCK // tp
    picked = jnp.zeros((BLOCK, LANE), jnp.float32)
    for k in range(tp):
        own = (lane == row - k * share) & (lane < share)
        picked = jnp.where(own, jnp.broadcast_to(nz[k], (BLOCK, LANE)), picked)
    column = jnp.sum(picked, axis=1, keepdims=True)
    tail = jnp.where(lane == HALF, column, tail)
    all_ref[mine, COLUMNS - LANE : COLUMNS] = tail.astype(jnp.bfloat16)
    here.add(("B1", 0, 0))
    issue()
    for chunk in CHUNKS:
        hand_over((chunk, 0, 0))

    for item in arrivals:
        if item[1:] == (0, 0):
            continue
        part = span(item)
        pltpu.make_async_remote_copy(
            src_ref=part, dst_ref=part, send_sem=send_sem, recv_sem=recv_sem.at[number[item]],
            device_id={"zero": peer, "tp": z}, device_id_type=MESH,
        ).wait_recv()
        here.add(item)
        issue()
        hand_over(item)
    assert not any(queue.values())

    blocks = SIDE * SIDE
    for sem, rows in ((peer_recv, blocks), (peer_send, blocks), (send_sem, blocks - 1)):
        whole = all_ref.at[0 : rows * BLOCK]
        pltpu.make_async_copy(whole, whole, sem).wait()
    for copy in norm_copies:
        copy.wait_send()


def turn_kernel(all_ref, gate, up, down, norm, stage, norm_rows, sem, norm_sem):
    outs = (gate, up, down)
    total = all_ref.shape[0]
    size, step = stage.shape[1], LANE
    starts = list(range(0, COLUMNS, size))
    pending = {}
    for order, start in enumerate(starts[-1:] + starts[:-1]):
        wide = min(size, COLUMNS - start)
        slot = order % stage.shape[0]
        for copy in pending.pop(slot, ()):
            copy.wait()

        def body(i, carry):
            rows = pl.ds(pl.multiple_of(i * step, step), step)
            stage[slot, 0:wide, rows] = all_ref[rows, start : start + wide].T
            return carry

        lax.fori_loop(0, total // step, body, 0, unroll=True)
        started = []
        for t in range(3):
            lo, hi = max(start, t * WIDTH), min(start + wide, (t + 1) * WIDTH)
            if lo < hi:
                copy = pltpu.make_async_copy(
                    stage.at[slot, lo - start : hi - start],
                    outs[t].at[lo - t * WIDTH : hi - t * WIDTH],
                    sem.at[slot, len(started)],
                )
                copy.start()
                started.append(copy)
        if start <= NORM_LANE < start + wide:
            row = stage[slot, NORM_LANE - start : NORM_LANE - start + 1, :].astype(jnp.float32)
            pieces = [row[:, k : k + LANE] for k in range(0, total, LANE)]
            norm_rows[...] = jnp.concatenate(pieces, axis=0).astype(jnp.bfloat16)
            copy = pltpu.make_async_copy(norm_rows, norm, norm_sem)
            copy.start()
            started.append(copy)
        pending[slot] = started
    for started in pending.values():
        for copy in started:
            copy.wait()


def local(wg, ag, bg, wu, au, bu, wd, ad, bd, nt, ns):
    rows = 2560
    bf16 = jnp.bfloat16
    hbm = pl.BlockSpec(memory_space=pltpu.HBM)
    inputs = (wg, ag.T, bg, wu, au.T, bu, wd.T, bd, ad.T, nt.reshape(1, -1), ns.reshape(1, -1))
    items = len(CHUNKS) * (SIDE * SIDE - 1)
    gathered = pl.pallas_call(
        gather_kernel,
        out_shape=pltpu.VMEM((rows, COLUMNS), bf16),
        in_specs=[hbm] * 11,
        out_specs=pl.BlockSpec(memory_space=pltpu.VMEM),
        scratch_shapes=[
            pltpu.VMEM((3, BLOCK, WIDTH), bf16),
            pltpu.VMEM((3, RANK, BLOCK), bf16),
            pltpu.VMEM((3, RANK, WIDTH), bf16),
            pltpu.VMEM((2, 1, nt.shape[0]), jnp.float32),
            pltpu.VMEM((8, 1, LANE), jnp.float32),
            pltpu.SemaphoreType.DMA((11,)),
            pltpu.SemaphoreType.DMA((items,)),
            pltpu.SemaphoreType.DMA((7,)),
            pltpu.SemaphoreType.DMA((7,)),
            pltpu.SemaphoreType.DMA,
            pltpu.SemaphoreType.DMA,
            pltpu.SemaphoreType.DMA,
        ],
        compiler_params=pltpu.CompilerParams(collective_id=0, has_side_effects=True, vmem_limit_bytes=16 << 20),
        name="gather",
    )(*(pltpu.with_memory_space_constraint(v, pltpu.HBM) for v in inputs))
    gate, up, down, norm = pl.pallas_call(
        turn_kernel,
        out_shape=[jax.ShapeDtypeStruct((WIDTH, rows), bf16)] * 3 + [jax.ShapeDtypeStruct((rows // LANE, LANE), bf16)],
        in_specs=[pl.BlockSpec(memory_space=pltpu.VMEM)],
        out_specs=[hbm] * 4,
        scratch_shapes=[
            pltpu.VMEM((4, 256, rows), bf16),
            pltpu.VMEM((rows // LANE, LANE), bf16),
            pltpu.SemaphoreType.DMA((4, 2)),
            pltpu.SemaphoreType.DMA,
        ],
        compiler_params=pltpu.CompilerParams(vmem_limit_bytes=16 << 20),
        name="turn",
    )(gathered)
    return gate.T, up.T, down, norm.reshape(rows)


def solution(mesh):
    return jax.shard_map(
        local,
        mesh=mesh,
        in_specs=(
            P("zero", "tp"),
            P("zero", None),
            P(None, "tp"),
            P("zero", "tp"),
            P("zero", None),
            P(None, "tp"),
            P("tp", "zero"),
            P("tp", None),
            P(None, "zero"),
            P(("zero", "tp")),
            P(("zero", "tp")),
        ),
        out_specs=(P(None, "tp"), P(None, "tp"), P("tp", None), P()),
        check_vma=False,
    )
```

```python
import functools
import heapq

import jax
import jax.numpy as jnp
from jax import lax
from jax.experimental import pallas as pl
from jax.experimental.pallas import tpu as pltpu
from jax.sharding import PartitionSpec as P

MESH = pl.DeviceIdType.MESH
LINKS = ("u+", "u-", "v+", "v-")
SIDE = 4
BLOCK = 80
WIDTH = 1216
RANK = 16
LANE = 128
CHUNKS = {"A0": (0, 7), "B1": (21, 28), "A1": (7, 14), "B0": (14, 21), "C0": (28, 29)}
OWN_US = {"A0": 0.0, "B1": 0.0, "A1": 0.6, "B0": 0.6, "C0": 20.0}
TILES = 29
COLUMNS = TILES * LANE
NORM_LANE = 3 * WIDTH
HALF = LANE // 2

mix_rate = 0.5


def onward(item):
    chunk, ou, ov = item
    first, second = ("v", "u") if chunk[0] == "B" else ("u", "v")
    a, b = (ov, ou) if chunk[0] == "B" else (ou, ov)
    turn = "+" if chunk[1] == "0" else "-"
    far = SIDE - 1 if turn == "+" else 1
    if b == 0:
        out = [first + "+", first + "-"] if a == 0 else [first + turn] if a == far else []
        return out + [second + "+", second + "-"]
    return [second + turn] if b == far else []


def seen_there(item, link):
    chunk, ou, ov = item
    step = SIDE - 1 if link[1] == "+" else 1
    return (chunk, (ou + step) % SIDE, ov) if link[0] == "u" else (chunk, ou, (ov + step) % SIDE)


def depth(item):
    return max((1 + depth(seen_there(item, link)) for link in onward(item)), default=0)


def plan(tile_us=0.44, hop_us=2.5):
    free = dict.fromkeys(LINKS, 0.0)
    ready = {link: [] for link in LINKS}
    sends = {link: [] for link in LINKS}
    arrivals, events, count = [], [], 0
    for chunk in CHUNKS:
        events.append((OWN_US[chunk], count, (chunk, 0, 0)))
        count += 1
    while events:
        now, _, item = heapq.heappop(events)
        if item is not None:
            arrivals.append(item)
            for link in onward(item):
                heapq.heappush(ready[link], (-depth(seen_there(item, link)), count, item))
                count += 1
        if events and events[0][0] <= now + 1e-9:
            continue
        for link in LINKS:
            if free[link] <= now + 1e-9 and ready[link]:
                item = heapq.heappop(ready[link])[2]
                lo, hi = CHUNKS[item[0]]
                free[link] = now + (hi - lo) * tile_us
                sends[link].append(item)
                heapq.heappush(events, (free[link], count, None))
                heapq.heappush(events, (free[link] + hop_us, count + 1, seen_there(item, link)))
                count += 2
    return sends, arrivals


def gather_kernel(
    wg, ag, bg, wu, au, bu, wd, ad, bd, nt, ns, all_ref,
    w, a, b, n, nz, in_sem, recv_sem, norm_send, norm_recv, ready, send_sem, peer_send, peer_recv,
):
    zero, z = lax.axis_index("zero"), lax.axis_index("tp")
    tp = lax.axis_size("tp")
    core, chip = lax.rem(zero, 2), lax.div(zero, 2)
    x, y = lax.rem(chip, SIDE), lax.div(chip, SIDE)

    def at(ou, ov):
        ox = lax.rem(x + (1 - core) * ou - core * ov + SIDE, SIDE)
        oy = lax.rem(y + (1 - core) * ov - core * ou + SIDE, SIDE)
        return (oy * SIDE + ox) * 2 + core

    place = {(ou, ov): at(ou, ov) for ou in range(SIDE) for ov in range(SIDE)}
    target = {"u+": place[1, 0], "u-": place[3, 0], "v+": place[0, 1], "v-": place[0, 3]}
    peer = zero + 1 - 2 * core

    loads = []
    for k, (src, dst) in enumerate(
        [
            pair
            for t, refs in ((0, (wg, ag, bg)), (2, (wd, ad, bd)), (1, (wu, au, bu)))
            for pair in zip(refs, (w.at[t], a.at[t], b.at[t]))
        ]
        + [(nt, n.at[0]), (ns, n.at[1])]
    ):
        load = pltpu.make_async_copy(src, dst, in_sem.at[k])
        load.start()
        loads.append(load)

    barrier = pltpu.get_barrier_semaphore()
    for other in list(target.values()) + [peer]:
        pl.semaphore_signal(barrier, inc=1, device_id={"zero": other, "tp": z}, device_id_type=MESH)
    for k in range(1, tp):

        @pl.when(k > z)
        def _():
            pl.semaphore_signal(barrier, inc=1, device_id={"zero": zero, "tp": k}, device_id_type=MESH)

    mine = pl.ds(pl.multiple_of(zero * BLOCK, 16), BLOCK)
    cut = WIDTH - HALF

    def latest(t, order):
        for load in loads[3 * order : 3 * order + 3]:
            load.wait()
        low_high = lax.dot_general(
            a[t], b[t], (((0,), (0,)), ((), ())), preferred_element_type=jnp.float32
        )
        return w[t].astype(jnp.float32) + mix_rate * low_high

    gate = latest(0, 0)
    all_ref[mine, 0:cut] = gate[:, :cut].astype(jnp.bfloat16)
    down = latest(2, 1)
    all_ref[mine, 2 * WIDTH : 2 * WIDTH + cut] = down[:, :cut].astype(jnp.bfloat16)

    sends, arrivals = plan()
    number = {item: k for k, item in enumerate(i for i in arrivals if i[1:] != (0, 0))}

    def span(item):
        chunk, ou, ov = item
        lo, hi = CHUNKS[chunk]
        rows = pl.ds(pl.multiple_of(place[ou, ov] * BLOCK, 16), BLOCK)
        return all_ref.at[rows, lo * LANE : hi * LANE]

    def send(item, link):
        part = span(item)
        pltpu.make_async_remote_copy(
            src_ref=part, dst_ref=part, send_sem=send_sem, recv_sem=recv_sem.at[number[seen_there(item, link)]],
            device_id={"zero": target[link], "tp": z}, device_id_type=MESH,
        ).start()

    def hand_over(item):
        part = span(item)
        pltpu.make_async_remote_copy(
            src_ref=part, dst_ref=part, send_sem=peer_send, recv_sem=peer_recv,
            device_id={"zero": peer, "tp": z}, device_id_type=MESH,
        ).start()

    queue = {link: list(order) for link, order in sends.items()}
    here = set()

    def issue(*items):
        here.update(items)
        moved = True
        while moved:
            moved = False
            for link in LINKS:
                if queue[link] and queue[link][0] in here:
                    send(queue[link].pop(0), link)
                    moved = True
        for item in items:
            hand_over(item)

    def norm_copy(k):
        return pltpu.make_async_remote_copy(
            src_ref=nz.at[z], dst_ref=nz.at[z], send_sem=norm_send.at[k], recv_sem=norm_recv.at[z],
            device_id={"zero": zero, "tp": k}, device_id_type=MESH,
        )

    pl.semaphore_wait(barrier, len(target) + 1 + z)
    issue(("A0", 0, 0), ("B1", 0, 0))

    up = latest(1, 2)
    both = jnp.concatenate([gate[:, cut:], up], axis=1)
    all_ref[mine, cut : 2 * WIDTH] = both.astype(jnp.bfloat16)
    loads[9].wait()
    loads[10].wait()
    gain = (n[0] + n[1]).astype(jnp.bfloat16).astype(jnp.float32)
    nz[z] = jnp.concatenate([gain, jnp.zeros((1, LANE - gain.shape[1]), jnp.float32)], axis=1)
    issue(("A1", 0, 0), ("B0", 0, 0))

    for k in range(tp - 1):

        @pl.when(k < z)
        def _():
            pl.semaphore_signal(ready, inc=1, device_id={"zero": zero, "tp": k}, device_id_type=MESH)
            norm_copy(k).start()

    waited = 0
    for item in arrivals:
        if item == ("C0", 0, 0):
            for k in range(tp):

                @pl.when(k != z)
                def _():
                    pltpu.make_async_remote_copy(
                        src_ref=nz.at[k], dst_ref=nz.at[k], send_sem=norm_send.at[k], recv_sem=norm_recv.at[k],
                        device_id={"zero": zero, "tp": k}, device_id_type=MESH,
                    ).wait_recv()

            row = lax.broadcasted_iota(jnp.int32, (BLOCK, LANE), 0)
            lane = lax.broadcasted_iota(jnp.int32, (BLOCK, LANE), 1)
            share = BLOCK // tp
            picked = jnp.zeros((BLOCK, LANE), jnp.float32)
            for k in range(tp):
                own = (lane == row - k * share) & (lane < share)
                picked = jnp.where(own, jnp.broadcast_to(nz[k], (BLOCK, LANE)), picked)
            column = jnp.sum(picked, axis=1, keepdims=True)
            tail = jnp.concatenate([down[:, cut:], jnp.zeros((BLOCK, HALF), jnp.float32)], axis=1)
            tail = jnp.where(lane == HALF, column, tail)
            all_ref[mine, COLUMNS - LANE : COLUMNS] = tail.astype(jnp.bfloat16)
            issue(item)
        elif item[1:] != (0, 0):
            part = span(item)
            pltpu.make_async_remote_copy(
                src_ref=part, dst_ref=part, send_sem=send_sem, recv_sem=recv_sem.at[number[item]],
                device_id={"zero": peer, "tp": z}, device_id_type=MESH,
            ).wait_recv()
            issue(item)
            waited += 1
            if waited == 8:

                @pl.when(z < tp - 1)
                def _():
                    pl.semaphore_wait(ready, tp - 1 - z)

                for k in range(1, tp):

                    @pl.when(k > z)
                    def _():
                        norm_copy(k).start()

    assert not any(queue.values())

    blocks = SIDE * SIDE
    for sem, rows in ((peer_recv, blocks), (peer_send, blocks), (send_sem, blocks - 1)):
        whole = all_ref.at[0 : rows * BLOCK]
        pltpu.make_async_copy(whole, whole, sem).wait()
    for k in range(tp):

        @pl.when(k != z)
        def _():
            norm_copy(k).wait_send()


def turn_kernel(all_ref, gate, up, down, norm, stage, norm_rows, sem, norm_sem):
    outs = (gate, up, down)
    total = all_ref.shape[0]
    size, step = stage.shape[1], LANE
    starts = list(range(0, COLUMNS, size))
    pending = {}
    for order, start in enumerate(starts[-1:] + starts[:-1]):
        wide = min(size, COLUMNS - start)
        slot = order % stage.shape[0]
        for copy in pending.pop(slot, ()):
            copy.wait()

        def body(i, carry):
            rows = pl.ds(pl.multiple_of(i * step, step), step)
            stage[slot, 0:wide, rows] = all_ref[rows, start : start + wide].T
            return carry

        lax.fori_loop(0, total // step, body, 0, unroll=True)
        started = []
        for t in range(3):
            lo, hi = max(start, t * WIDTH), min(start + wide, (t + 1) * WIDTH)
            if lo < hi:
                copy = pltpu.make_async_copy(
                    stage.at[slot, lo - start : hi - start],
                    outs[t].at[lo - t * WIDTH : hi - t * WIDTH],
                    sem.at[slot, len(started)],
                )
                copy.start()
                started.append(copy)
        if start <= NORM_LANE < start + wide:
            row = stage[slot, NORM_LANE - start : NORM_LANE - start + 1, :].astype(jnp.float32)
            pieces = [row[:, k : k + LANE] for k in range(0, total, LANE)]
            norm_rows[...] = jnp.concatenate(pieces, axis=0).astype(jnp.bfloat16)
            copy = pltpu.make_async_copy(norm_rows, norm, norm_sem)
            copy.start()
            started.append(copy)
        pending[slot] = started
    for started in pending.values():
        for copy in started:
            copy.wait()


def local(wg, ag, bg, wu, au, bu, wd, ad, bd, nt, ns):
    rows = 2560
    bf16 = jnp.bfloat16
    hbm = pl.BlockSpec(memory_space=pltpu.HBM)
    inputs = (wg, ag.T, bg, wu, au.T, bu, wd.T, bd, ad.T, nt.reshape(1, -1), ns.reshape(1, -1))
    items = len(CHUNKS) * (SIDE * SIDE - 1)
    gathered = pl.pallas_call(
        gather_kernel,
        out_shape=pltpu.VMEM((rows, COLUMNS), bf16),
        in_specs=[hbm] * 11,
        out_specs=pl.BlockSpec(memory_space=pltpu.VMEM),
        scratch_shapes=[
            pltpu.VMEM((3, BLOCK, WIDTH), bf16),
            pltpu.VMEM((3, RANK, BLOCK), bf16),
            pltpu.VMEM((3, RANK, WIDTH), bf16),
            pltpu.VMEM((2, 1, nt.shape[0]), jnp.float32),
            pltpu.VMEM((8, 1, LANE), jnp.float32),
            pltpu.SemaphoreType.DMA((11,)),
            pltpu.SemaphoreType.DMA((items,)),
            pltpu.SemaphoreType.DMA((8,)),
            pltpu.SemaphoreType.DMA((8,)),
            pltpu.SemaphoreType.REGULAR,
            pltpu.SemaphoreType.DMA,
            pltpu.SemaphoreType.DMA,
            pltpu.SemaphoreType.DMA,
        ],
        compiler_params=pltpu.CompilerParams(collective_id=0, has_side_effects=True, vmem_limit_bytes=16 << 20),
        name="gather",
    )(*(pltpu.with_memory_space_constraint(v, pltpu.HBM) for v in inputs))
    gate, up, down, norm = pl.pallas_call(
        turn_kernel,
        out_shape=[jax.ShapeDtypeStruct((WIDTH, rows), bf16)] * 3 + [jax.ShapeDtypeStruct((rows // LANE, LANE), bf16)],
        in_specs=[pl.BlockSpec(memory_space=pltpu.VMEM)],
        out_specs=[hbm] * 4,
        scratch_shapes=[
            pltpu.VMEM((4, 256, rows), bf16),
            pltpu.VMEM((rows // LANE, LANE), bf16),
            pltpu.SemaphoreType.DMA((4, 2)),
            pltpu.SemaphoreType.DMA,
        ],
        compiler_params=pltpu.CompilerParams(vmem_limit_bytes=16 << 20),
        name="turn",
    )(gathered)
    return gate.T, up.T, down, norm.reshape(rows)


def solution(mesh):
    return jax.shard_map(
        local,
        mesh=mesh,
        in_specs=(
            P("zero", "tp"),
            P("zero", None),
            P(None, "tp"),
            P("zero", "tp"),
            P("zero", None),
            P(None, "tp"),
            P("tp", "zero"),
            P("tp", None),
            P(None, "zero"),
            P(("zero", "tp")),
            P(("zero", "tp")),
        ),
        out_specs=(P(None, "tp"), P(None, "tp"), P("tp", None), P()),
        check_vma=False,
    )
```

```python
import functools
import heapq

import jax
import jax.numpy as jnp
from jax import lax
from jax.experimental import pallas as pl
from jax.experimental.pallas import tpu as pltpu
from jax.sharding import PartitionSpec as P

MESH = pl.DeviceIdType.MESH
LINKS = ("u+", "u-", "v+", "v-")
SIDE = 4
BLOCK = 80
WIDTH = 1216
RANK = 16
LANE = 128
CHUNKS = {"A0": (0, 7), "B1": (21, 28), "A1": (7, 14), "B0": (14, 21), "C0": None}
OWN_US = {"A0": 0.0, "B1": 0.0, "A1": 0.6, "B0": 0.6, "C0": 15.0}
COLUMNS = 28 * LANE
HALF = LANE // 2
FOLD = 48

mix_rate = 0.5


def onward(item):
    chunk, ou, ov = item
    first, second = ("v", "u") if chunk[0] == "B" else ("u", "v")
    a, b = (ov, ou) if chunk[0] == "B" else (ou, ov)
    turn = "+" if chunk[1] == "0" else "-"
    far = SIDE - 1 if turn == "+" else 1
    if b == 0:
        out = [first + "+", first + "-"] if a == 0 else [first + turn] if a == far else []
        return out + [second + "+", second + "-"]
    return [second + turn] if b == far else []


def seen_there(item, link):
    chunk, ou, ov = item
    step = SIDE - 1 if link[1] == "+" else 1
    return (chunk, (ou + step) % SIDE, ov) if link[0] == "u" else (chunk, ou, (ov + step) % SIDE)


def depth(item):
    return max((1 + depth(seen_there(item, link)) for link in onward(item)), default=0)


def plan(tile_us=0.44, hop_us=2.5):
    free = dict.fromkeys(LINKS, 0.0)
    ready = {link: [] for link in LINKS}
    sends = {link: [] for link in LINKS}
    arrivals, events, count = [], [], 0
    for chunk in CHUNKS:
        events.append((OWN_US[chunk], count, (chunk, 0, 0)))
        count += 1
    while events:
        now, _, item = heapq.heappop(events)
        if item is not None:
            arrivals.append(item)
            for link in onward(item):
                urgent = depth(seen_there(item, link)) if CHUNKS[item[0]] else 9
                heapq.heappush(ready[link], (-urgent, count, item))
                count += 1
        if events and events[0][0] <= now + 1e-9:
            continue
        for link in LINKS:
            if free[link] <= now + 1e-9 and ready[link]:
                item = heapq.heappop(ready[link])[2]
                lo, hi = CHUNKS[item[0]] or (0, 0.6)
                free[link] = now + (hi - lo) * tile_us
                sends[link].append(item)
                heapq.heappush(events, (free[link], count, None))
                heapq.heappush(events, (free[link] + hop_us, count + 1, seen_there(item, link)))
                count += 2
    return sends, arrivals


def gather_kernel(
    wg, ag, bg, wu, au, bu, wd, ad, bd, nt, ns, all_ref, rest, norm,
    w, a, b, n, nz, folded, picks, flat,
    in_sem, recv_sem, norm_send, norm_recv, ready, send_sem, peer_send, peer_recv,
):
    zero, z = lax.axis_index("zero"), lax.axis_index("tp")
    tp = lax.axis_size("tp")
    core, chip = lax.rem(zero, 2), lax.div(zero, 2)
    x, y = lax.rem(chip, SIDE), lax.div(chip, SIDE)

    def at(ou, ov):
        ox = lax.rem(x + (1 - core) * ou - core * ov + SIDE, SIDE)
        oy = lax.rem(y + (1 - core) * ov - core * ou + SIDE, SIDE)
        return (oy * SIDE + ox) * 2 + core

    place = {(ou, ov): at(ou, ov) for ou in range(SIDE) for ov in range(SIDE)}
    target = {"u+": place[1, 0], "u-": place[3, 0], "v+": place[0, 1], "v-": place[0, 3]}
    peer = zero + 1 - 2 * core

    loads = []
    for k, (src, dst) in enumerate(
        [
            pair
            for t, refs in ((0, (wg, ag, bg)), (2, (wd, ad, bd)), (1, (wu, au, bu)))
            for pair in zip(refs, (w.at[t], a.at[t], b.at[t]))
        ]
        + [(nt, n.at[0]), (ns, n.at[1])]
    ):
        load = pltpu.make_async_copy(src, dst, in_sem.at[k])
        load.start()
        loads.append(load)

    barrier = pltpu.get_barrier_semaphore()
    for other in list(target.values()) + [peer]:
        pl.semaphore_signal(barrier, inc=1, device_id={"zero": other, "tp": z}, device_id_type=MESH)
    for k in range(1, tp):

        @pl.when(k > z)
        def _():
            pl.semaphore_signal(barrier, inc=1, device_id={"zero": zero, "tp": k}, device_id_type=MESH)

    mine = pl.ds(pl.multiple_of(zero * BLOCK, 16), BLOCK)
    cut = WIDTH - HALF

    def latest(t, order):
        for load in loads[3 * order : 3 * order + 3]:
            load.wait()
        low_high = lax.dot_general(
            a[t], b[t], (((0,), (0,)), ((), ())), preferred_element_type=jnp.float32
        )
        return w[t].astype(jnp.float32) + mix_rate * low_high

    gate = latest(0, 0)
    all_ref[mine, 0:cut] = gate[:, :cut].astype(jnp.bfloat16)
    down = latest(2, 1)
    all_ref[mine, 2 * WIDTH : 2 * WIDTH + cut] = down[:, :cut].astype(jnp.bfloat16)

    sends, arrivals = plan()
    number = {item: k for k, item in enumerate(i for i in arrivals if i[1:] != (0, 0))}

    def kind(item):
        return int(CHUNKS[item[0]] is None)

    def span(item):
        chunk, ou, ov = item
        if CHUNKS[chunk] is None:
            return folded.at[pl.ds(pl.multiple_of(place[ou, ov] * FOLD, 16), FOLD)]
        lo, hi = CHUNKS[chunk]
        rows = pl.ds(pl.multiple_of(place[ou, ov] * BLOCK, 16), BLOCK)
        return all_ref.at[rows, lo * LANE : hi * LANE]

    def send(item, link):
        part = span(item)
        pltpu.make_async_remote_copy(
            src_ref=part, dst_ref=part, send_sem=send_sem.at[kind(item)], recv_sem=recv_sem.at[number[seen_there(item, link)]],
            device_id={"zero": target[link], "tp": z}, device_id_type=MESH,
        ).start()

    def hand_over(item):
        part = span(item)
        pltpu.make_async_remote_copy(
            src_ref=part, dst_ref=part, send_sem=peer_send.at[kind(item)], recv_sem=peer_recv.at[kind(item)],
            device_id={"zero": peer, "tp": z}, device_id_type=MESH,
        ).start()

    queue = {link: list(order) for link, order in sends.items()}
    here = set()

    def issue(*items):
        here.update(items)
        moved = True
        while moved:
            moved = False
            for link in LINKS:
                if queue[link] and queue[link][0] in here:
                    send(queue[link].pop(0), link)
                    moved = True
        for item in items:
            hand_over(item)

    def norm_copy(k):
        return pltpu.make_async_remote_copy(
            src_ref=nz.at[z], dst_ref=nz.at[z], send_sem=norm_send.at[k], recv_sem=norm_recv.at[z],
            device_id={"zero": zero, "tp": k}, device_id_type=MESH,
        )

    pl.semaphore_wait(barrier, len(target) + 1 + z)
    issue(("A0", 0, 0), ("B1", 0, 0))

    up = latest(1, 2)
    both = jnp.concatenate([gate[:, cut:], up], axis=1)
    all_ref[mine, cut : 2 * WIDTH] = both.astype(jnp.bfloat16)
    loads[9].wait()
    loads[10].wait()
    gain = (n[0] + n[1]).astype(jnp.bfloat16).astype(jnp.float32)
    nz[z] = jnp.concatenate([gain, jnp.zeros((1, LANE - gain.shape[1]), jnp.float32)], axis=1)
    issue(("A1", 0, 0), ("B0", 0, 0))

    for k in range(tp - 1):

        @pl.when(k < z)
        def _():
            pl.semaphore_signal(ready, inc=1, device_id={"zero": zero, "tp": k}, device_id_type=MESH)
            norm_copy(k).start()

    wide = 8 * BLOCK

    def make_picks():
        for e in range(8):
            r = lax.broadcasted_iota(jnp.int32, (FOLD, wide), 0)
            c = lax.broadcasted_iota(jnp.int32, (FOLD, wide), 1) - e * BLOCK
            half = BLOCK // 2
            for m, hit in enumerate(
                [(c == r) & (r < half), (c == r + half) & (r < half), (r == half) & (c >= 0) & (c < BLOCK)]
            ):
                picks[m, e * FOLD : (e + 1) * FOLD] = jnp.where(hit, 1.0, 0.0).astype(jnp.bfloat16)

    def unfold(g):
        rows = folded[g * 8 * FOLD : (g + 1) * 8 * FOLD]
        left, right, line = (
            lax.dot_general(rows, picks[m], (((0,), (0,)), ((), ())), preferred_element_type=jnp.float32)
            for m in range(3)
        )
        rest[:, g * wide : (g + 1) * wide] = (left[:HALF] + right[HALF:]).astype(jnp.bfloat16)
        i = lax.broadcasted_iota(jnp.int32, (BLOCK, wide), 0)
        l = lax.broadcasted_iota(jnp.int32, (BLOCK, wide), 1)
        own = functools.reduce(jnp.logical_or, [i + e * BLOCK == l for e in range(8)])
        gains = jnp.sum(jnp.where(own, line[:BLOCK], 0.0), axis=0, keepdims=True)
        for k in range(wide // LANE):
            at_row = g * (wide // LANE) + k
            flat[at_row : at_row + 1] = gains[:, k * LANE : (k + 1) * LANE]

    c_left = sum(kind(item) for item in arrivals) - 1
    groups = list(range(all_ref.shape[0] // wide))
    waited, stored = 0, []
    for item in arrivals:
        if item == ("C0", 0, 0):
            for k in range(tp):

                @pl.when(k != z)
                def _():
                    pltpu.make_async_remote_copy(
                        src_ref=nz.at[k], dst_ref=nz.at[k], send_sem=norm_send.at[k], recv_sem=norm_recv.at[k],
                        device_id={"zero": zero, "tp": k}, device_id_type=MESH,
                    ).wait_recv()

            share = BLOCK // tp
            gains = [nz[k][:, :share] for k in range(tp)] + [jnp.zeros((1, LANE - BLOCK), jnp.float32)]
            gains = jnp.concatenate(gains, axis=1)
            left = down[:, cut:]
            top = jnp.concatenate([left[: BLOCK // 2], left[BLOCK // 2 :]], axis=1)
            line = lax.broadcasted_iota(jnp.int32, (FOLD - BLOCK // 2, LANE), 0)
            bottom = jnp.where(line == 0, jnp.broadcast_to(gains, line.shape), 0.0)
            fold = jnp.concatenate([top, bottom], axis=0).astype(jnp.bfloat16)
            folded[pl.ds(pl.multiple_of(zero * FOLD, 16), FOLD)] = fold
            stored.append(item)
        elif item[1:] != (0, 0):
            part = span(item)
            pltpu.make_async_remote_copy(
                src_ref=part, dst_ref=part, send_sem=send_sem.at[kind(item)], recv_sem=recv_sem.at[number[item]],
                device_id={"zero": peer, "tp": z}, device_id_type=MESH,
            ).wait_recv()
            issue(item, *stored)
            stored.clear()
            waited += 1
            c_left -= kind(item)
            if waited == 6:
                make_picks()
            if c_left == 0 and kind(item):
                folds = folded.at[0 : SIDE * SIDE * FOLD]
                pltpu.make_async_copy(folds, folds, peer_recv.at[1]).wait()
            elif c_left == 0 and groups:
                unfold(groups.pop(0))
            if waited == 8:

                @pl.when(z < tp - 1)
                def _():
                    pl.semaphore_wait(ready, tp - 1 - z)

                for k in range(1, tp):

                    @pl.when(k > z)
                    def _():
                        norm_copy(k).start()

    assert not any(queue.values()) and not groups

    norm[...] = flat[0 : norm.shape[0]].astype(jnp.bfloat16)
    blocks = SIDE * SIDE
    for sem, count, buffer, rows in (
        (peer_recv.at[0], blocks, all_ref, BLOCK),
        (peer_send.at[0], blocks, all_ref, BLOCK),
        (peer_send.at[1], blocks, folded, FOLD),
        (send_sem.at[0], blocks - 1, all_ref, BLOCK),
        (send_sem.at[1], blocks - 1, folded, FOLD),
    ):
        whole = buffer.at[0 : count * rows]
        pltpu.make_async_copy(whole, whole, sem).wait()
    for k in range(tp):

        @pl.when(k != z)
        def _():
            norm_copy(k).wait_send()


def turn_kernel(all_ref, rest, norm_rows, gate, up, down, norm, stage, sem, rest_sem):
    outs = (gate, up, down)
    total = all_ref.shape[0]
    size, step = stage.shape[1], LANE
    lasts = [
        pltpu.make_async_copy(rest, down.at[WIDTH - HALF : WIDTH], rest_sem.at[0]),
        pltpu.make_async_copy(norm_rows, norm, rest_sem.at[1]),
    ]
    for copy in lasts:
        copy.start()
    pending = {}
    for order, start in enumerate(range(0, COLUMNS, size)):
        slot = order % stage.shape[0]
        for copy in pending.pop(slot, ()):
            copy.wait()

        def body(i, carry):
            rows = pl.ds(pl.multiple_of(i * step, step), step)
            stage[slot, :, rows] = all_ref[rows, start : start + size].T
            return carry

        lax.fori_loop(0, total // step, body, 0, unroll=True)
        started = []
        for t in range(3):
            lo, hi = max(start, t * WIDTH), min(start + size, (t + 1) * WIDTH)
            if lo < hi:
                copy = pltpu.make_async_copy(
                    stage.at[slot, lo - start : hi - start],
                    outs[t].at[lo - t * WIDTH : hi - t * WIDTH],
                    sem.at[slot, len(started)],
                )
                copy.start()
                started.append(copy)
        pending[slot] = started
    for started in [lasts, *pending.values()]:
        for copy in started:
            copy.wait()


def local(wg, ag, bg, wu, au, bu, wd, ad, bd, nt, ns):
    rows = 2560
    bf16 = jnp.bfloat16
    hbm = pl.BlockSpec(memory_space=pltpu.HBM)
    inputs = (wg, ag.T, bg, wu, au.T, bu, wd.T, bd, ad.T, nt.reshape(1, -1), ns.reshape(1, -1))
    items = len(CHUNKS) * (SIDE * SIDE - 1)
    vmem = pl.BlockSpec(memory_space=pltpu.VMEM)
    flat_rows = rows // LANE
    gathered = pl.pallas_call(
        gather_kernel,
        out_shape=[
            pltpu.VMEM((rows, COLUMNS), bf16),
            pltpu.VMEM((HALF, rows), bf16),
            pltpu.VMEM((flat_rows, LANE), bf16),
        ],
        in_specs=[hbm] * 11,
        out_specs=[vmem] * 3,
        scratch_shapes=[
            pltpu.VMEM((3, BLOCK, WIDTH), bf16),
            pltpu.VMEM((3, RANK, BLOCK), bf16),
            pltpu.VMEM((3, RANK, WIDTH), bf16),
            pltpu.VMEM((2, 1, nt.shape[0]), jnp.float32),
            pltpu.VMEM((8, 1, LANE), jnp.float32),
            pltpu.VMEM((2 * SIDE * SIDE * FOLD, LANE), bf16),
            pltpu.VMEM((3, 8 * FOLD, 8 * BLOCK), bf16),
            pltpu.VMEM((24, LANE), jnp.float32),
            pltpu.SemaphoreType.DMA((11,)),
            pltpu.SemaphoreType.DMA((items,)),
            pltpu.SemaphoreType.DMA((8,)),
            pltpu.SemaphoreType.DMA((8,)),
            pltpu.SemaphoreType.REGULAR,
            pltpu.SemaphoreType.DMA((2,)),
            pltpu.SemaphoreType.DMA((2,)),
            pltpu.SemaphoreType.DMA((2,)),
        ],
        compiler_params=pltpu.CompilerParams(collective_id=0, has_side_effects=True, vmem_limit_bytes=16 << 20),
        name="gather",
    )(*(pltpu.with_memory_space_constraint(v, pltpu.HBM) for v in inputs))
    gate, up, down, norm = pl.pallas_call(
        turn_kernel,
        out_shape=[jax.ShapeDtypeStruct((WIDTH, rows), bf16)] * 3 + [jax.ShapeDtypeStruct((flat_rows, LANE), bf16)],
        in_specs=[vmem] * 3,
        out_specs=[hbm] * 4,
        scratch_shapes=[
            pltpu.VMEM((4, 256, rows), bf16),
            pltpu.SemaphoreType.DMA((4, 2)),
            pltpu.SemaphoreType.DMA((2,)),
        ],
        compiler_params=pltpu.CompilerParams(vmem_limit_bytes=16 << 20),
        name="turn",
    )(*gathered)
    return gate.T, up.T, down, norm.reshape(rows)


def solution(mesh):
    return jax.shard_map(
        local,
        mesh=mesh,
        in_specs=(
            P("zero", "tp"),
            P("zero", None),
            P(None, "tp"),
            P("zero", "tp"),
            P("zero", None),
            P(None, "tp"),
            P("tp", "zero"),
            P("tp", None),
            P(None, "zero"),
            P(("zero", "tp")),
            P(("zero", "tp")),
        ),
        out_specs=(P(None, "tp"), P(None, "tp"), P("tp", None), P()),
        check_vma=False,
    )
```

```python
import functools
import heapq

import jax
import jax.numpy as jnp
from jax import lax
from jax.experimental import pallas as pl
from jax.experimental.pallas import tpu as pltpu
from jax.sharding import PartitionSpec as P

MESH = pl.DeviceIdType.MESH
LINKS = ("u+", "u-", "v+", "v-")
SIDE = 4
BLOCK = 80
WIDTH = 1216
RANK = 16
LANE = 128
CHUNKS = {"A0": (0, 7), "B1": (21, 28), "A1": (7, 14), "B0": (14, 21), "C0": None}
OWN_US = {"A0": 0.0, "B1": 0.0, "A1": 0.6, "B0": 0.6, "C0": 15.0}
COLUMNS = 28 * LANE
HALF = LANE // 2
FOLD = 48

mix_rate = 0.5


def onward(item):
    chunk, ou, ov = item
    first, second = ("v", "u") if chunk[0] == "B" else ("u", "v")
    a, b = (ov, ou) if chunk[0] == "B" else (ou, ov)
    turn = "+" if chunk[1] == "0" else "-"
    far = SIDE - 1 if turn == "+" else 1
    if b == 0:
        out = [first + "+", first + "-"] if a == 0 else [first + turn] if a == far else []
        return out + [second + "+", second + "-"]
    return [second + turn] if b == far else []


def seen_there(item, link):
    chunk, ou, ov = item
    step = SIDE - 1 if link[1] == "+" else 1
    return (chunk, (ou + step) % SIDE, ov) if link[0] == "u" else (chunk, ou, (ov + step) % SIDE)


def depth(item):
    return max((1 + depth(seen_there(item, link)) for link in onward(item)), default=0)


def plan(tile_us=0.44, hop_us=4.0):
    free = dict.fromkeys(LINKS, 0.0)
    ready = {link: [] for link in LINKS}
    sends = {link: [] for link in LINKS}
    arrivals, events, count = [], [], 0
    for chunk in CHUNKS:
        events.append((OWN_US[chunk], count, (chunk, 0, 0)))
        count += 1
    while events:
        now, _, item = heapq.heappop(events)
        if item is not None:
            arrivals.append(item)
            for link in onward(item):
                urgent = depth(seen_there(item, link)) if CHUNKS[item[0]] else 9
                heapq.heappush(ready[link], (-urgent, count, item))
                count += 1
        if events and events[0][0] <= now + 1e-9:
            continue
        for link in LINKS:
            if free[link] <= now + 1e-9 and ready[link]:
                item = heapq.heappop(ready[link])[2]
                lo, hi = CHUNKS[item[0]] or (0, 0.6)
                free[link] = now + (hi - lo) * tile_us
                sends[link].append(item)
                heapq.heappush(events, (free[link], count, None))
                heapq.heappush(events, (free[link] + hop_us, count + 1, seen_there(item, link)))
                count += 2
    return sends, arrivals


def gather_kernel(
    wg, ag, bg, wu, au, bu, wd, ad, bd, nt, ns, all_ref, rest, norm,
    w, a, b, n, nz, folded, picks, flat,
    in_sem, recv_sem, norm_send, norm_recv, ready, send_sem, peer_send, peer_recv,
):
    zero, z = lax.axis_index("zero"), lax.axis_index("tp")
    tp = lax.axis_size("tp")
    core, chip = lax.rem(zero, 2), lax.div(zero, 2)
    x, y = lax.rem(chip, SIDE), lax.div(chip, SIDE)

    def at(ou, ov):
        ox = lax.rem(x + (1 - core) * ou - core * ov + SIDE, SIDE)
        oy = lax.rem(y + (1 - core) * ov - core * ou + SIDE, SIDE)
        return (oy * SIDE + ox) * 2 + core

    place = {(ou, ov): at(ou, ov) for ou in range(SIDE) for ov in range(SIDE)}
    target = {"u+": place[1, 0], "u-": place[3, 0], "v+": place[0, 1], "v-": place[0, 3]}
    peer = zero + 1 - 2 * core

    barrier = pltpu.get_barrier_semaphore()
    for other in list(target.values()) + [peer]:
        pl.semaphore_signal(barrier, inc=1, device_id={"zero": other, "tp": z}, device_id_type=MESH)
    for k in range(1, tp):

        @pl.when(k > z)
        def _():
            pl.semaphore_signal(barrier, inc=1, device_id={"zero": zero, "tp": k}, device_id_type=MESH)

    loads = []
    for k, (src, dst) in enumerate(
        [
            pair
            for t, refs in ((0, (wg, ag, bg)), (2, (wd, ad, bd)), (1, (wu, au, bu)))
            for pair in zip(refs, (w.at[t], a.at[t], b.at[t]))
        ]
        + [(nt, n.at[0]), (ns, n.at[1])]
    ):
        load = pltpu.make_async_copy(src, dst, in_sem.at[k])
        load.start()
        loads.append(load)

    mine = pl.ds(pl.multiple_of(zero * BLOCK, 16), BLOCK)
    cut = WIDTH - HALF

    def latest(t, lo, hi):
        low_high = lax.dot_general(
            a[t], b[t, :, lo:hi], (((0,), (0,)), ((), ())), preferred_element_type=jnp.float32
        )
        return w[t, :, lo:hi].astype(jnp.float32) + mix_rate * low_high

    def keep(first, value):
        all_ref[mine, first : first + value.shape[1]] = value.astype(jnp.bfloat16)

    def arrive(order):
        for load in loads[3 * order : 3 * order + 3]:
            load.wait()

    head = CHUNKS["A0"][1] * LANE
    back = CHUNKS["B1"][0] * LANE - 2 * WIDTH
    arrive(0)
    keep(0, latest(0, 0, head))
    arrive(1)
    keep(2 * WIDTH + back, latest(2, back, cut))

    sends, arrivals = plan()
    number = {item: k for k, item in enumerate(i for i in arrivals if i[1:] != (0, 0))}

    def kind(item):
        return int(CHUNKS[item[0]] is None)

    def span(item):
        chunk, ou, ov = item
        if CHUNKS[chunk] is None:
            return folded.at[pl.ds(pl.multiple_of(place[ou, ov] * FOLD, 16), FOLD)]
        lo, hi = CHUNKS[chunk]
        rows = pl.ds(pl.multiple_of(place[ou, ov] * BLOCK, 16), BLOCK)
        return all_ref.at[rows, lo * LANE : hi * LANE]

    def send(item, link):
        part = span(item)
        pltpu.make_async_remote_copy(
            src_ref=part, dst_ref=part, send_sem=send_sem.at[kind(item)], recv_sem=recv_sem.at[number[seen_there(item, link)]],
            device_id={"zero": target[link], "tp": z}, device_id_type=MESH,
        ).start()

    def hand_over(item):
        part = span(item)
        pltpu.make_async_remote_copy(
            src_ref=part, dst_ref=part, send_sem=peer_send.at[kind(item)], recv_sem=peer_recv.at[kind(item)],
            device_id={"zero": peer, "tp": z}, device_id_type=MESH,
        ).start()

    queue = {link: list(order) for link, order in sends.items()}
    here = set()

    def issue(*items):
        here.update(items)
        moved = True
        while moved:
            moved = False
            for link in LINKS:
                if queue[link] and queue[link][0] in here:
                    send(queue[link].pop(0), link)
                    moved = True
        for item in items:
            hand_over(item)

    def norm_copy(k):
        return pltpu.make_async_remote_copy(
            src_ref=nz.at[z], dst_ref=nz.at[z], send_sem=norm_send.at[k], recv_sem=norm_recv.at[z],
            device_id={"zero": zero, "tp": k}, device_id_type=MESH,
        )

    pl.semaphore_wait(barrier, len(target) + 1 + z)
    issue(("A0", 0, 0), ("B1", 0, 0))

    keep(2 * WIDTH, latest(2, 0, back))
    arrive(2)
    keep(head, jnp.concatenate([latest(0, head, WIDTH), latest(1, 0, WIDTH)], axis=1))
    loads[9].wait()
    loads[10].wait()
    gain = (n[0] + n[1]).astype(jnp.bfloat16).astype(jnp.float32)
    nz[z] = jnp.concatenate([gain, jnp.zeros((1, LANE - gain.shape[1]), jnp.float32)], axis=1)
    issue(("A1", 0, 0), ("B0", 0, 0))

    for k in range(tp - 1):

        @pl.when(k < z)
        def _():
            pl.semaphore_signal(ready, inc=1, device_id={"zero": zero, "tp": k}, device_id_type=MESH)
            norm_copy(k).start()

    wide = 8 * BLOCK

    def make_picks():
        for e in range(8):
            r = lax.broadcasted_iota(jnp.int32, (FOLD, wide), 0)
            c = lax.broadcasted_iota(jnp.int32, (FOLD, wide), 1) - e * BLOCK
            half = BLOCK // 2
            for m, hit in enumerate(
                [(c == r) & (r < half), (c == r + half) & (r < half), (r == half) & (c >= 0) & (c < BLOCK)]
            ):
                picks[m, e * FOLD : (e + 1) * FOLD] = jnp.where(hit, 1.0, 0.0).astype(jnp.bfloat16)

    def unfold(g):
        rows = folded[g * 8 * FOLD : (g + 1) * 8 * FOLD]
        left, right, line = (
            lax.dot_general(rows, picks[m], (((0,), (0,)), ((), ())), preferred_element_type=jnp.float32)
            for m in range(3)
        )
        rest[:, g * wide : (g + 1) * wide] = (left[:HALF] + right[HALF:]).astype(jnp.bfloat16)
        i = lax.broadcasted_iota(jnp.int32, (BLOCK, wide), 0)
        l = lax.broadcasted_iota(jnp.int32, (BLOCK, wide), 1)
        own = functools.reduce(jnp.logical_or, [i + e * BLOCK == l for e in range(8)])
        gains = jnp.sum(jnp.where(own, line[:BLOCK], 0.0), axis=0, keepdims=True)
        for k in range(wide // LANE):
            at_row = g * (wide // LANE) + k
            flat[at_row : at_row + 1] = gains[:, k * LANE : (k + 1) * LANE]

    c_left = sum(kind(item) for item in arrivals) - 1
    groups = list(range(all_ref.shape[0] // wide))
    waited, stored = 0, []
    for item in arrivals:
        if item == ("C0", 0, 0):
            for k in range(tp):

                @pl.when(k != z)
                def _():
                    pltpu.make_async_remote_copy(
                        src_ref=nz.at[k], dst_ref=nz.at[k], send_sem=norm_send.at[k], recv_sem=norm_recv.at[k],
                        device_id={"zero": zero, "tp": k}, device_id_type=MESH,
                    ).wait_recv()

            share = BLOCK // tp
            gains = [nz[k][:, :share] for k in range(tp)] + [jnp.zeros((1, LANE - BLOCK), jnp.float32)]
            gains = jnp.concatenate(gains, axis=1)
            left = latest(2, cut, WIDTH)
            top = jnp.concatenate([left[: BLOCK // 2], left[BLOCK // 2 :]], axis=1)
            line = lax.broadcasted_iota(jnp.int32, (FOLD - BLOCK // 2, LANE), 0)
            bottom = jnp.where(line == 0, jnp.broadcast_to(gains, line.shape), 0.0)
            fold = jnp.concatenate([top, bottom], axis=0).astype(jnp.bfloat16)
            folded[pl.ds(pl.multiple_of(zero * FOLD, 16), FOLD)] = fold
            stored.append(item)
        elif item[1:] != (0, 0):
            part = span(item)
            pltpu.make_async_remote_copy(
                src_ref=part, dst_ref=part, send_sem=send_sem.at[kind(item)], recv_sem=recv_sem.at[number[item]],
                device_id={"zero": peer, "tp": z}, device_id_type=MESH,
            ).wait_recv()
            issue(item, *stored)
            stored.clear()
            waited += 1
            c_left -= kind(item)
            if waited == 6:
                make_picks()
            if c_left == 0 and kind(item):
                folds = folded.at[0 : SIDE * SIDE * FOLD]
                pltpu.make_async_copy(folds, folds, peer_recv.at[1]).wait()
            elif c_left == 0 and groups:
                unfold(groups.pop(0))
            if waited == 8:

                @pl.when(z < tp - 1)
                def _():
                    pl.semaphore_wait(ready, tp - 1 - z)

                for k in range(1, tp):

                    @pl.when(k > z)
                    def _():
                        norm_copy(k).start()

    assert not any(queue.values()) and not groups

    norm[...] = flat[0 : norm.shape[0]].astype(jnp.bfloat16)
    blocks = SIDE * SIDE
    for sem, count, buffer, rows in (
        (peer_recv.at[0], blocks, all_ref, BLOCK),
        (peer_send.at[0], blocks, all_ref, BLOCK),
        (peer_send.at[1], blocks, folded, FOLD),
        (send_sem.at[0], blocks - 1, all_ref, BLOCK),
        (send_sem.at[1], blocks - 1, folded, FOLD),
    ):
        whole = buffer.at[0 : count * rows]
        pltpu.make_async_copy(whole, whole, sem).wait()
    for k in range(tp):

        @pl.when(k != z)
        def _():
            norm_copy(k).wait_send()


def turn_kernel(all_ref, rest, norm_rows, gate, up, down, norm, stage, sem, rest_sem):
    outs = (gate, up, down)
    total = all_ref.shape[0]
    size, step = stage.shape[1], LANE
    lasts = [
        pltpu.make_async_copy(rest, down.at[WIDTH - HALF : WIDTH], rest_sem.at[0]),
        pltpu.make_async_copy(norm_rows, norm, rest_sem.at[1]),
    ]
    for copy in lasts:
        copy.start()
    pending = {}
    half = size // 2
    blocks = [(0, half), (half, half)] + [(start, size) for start in range(size, COLUMNS, size)]
    for order, (start, wide) in enumerate(blocks):
        slot = order % stage.shape[0]
        for copy in pending.pop(slot, ()):
            copy.wait()

        def body(i, carry):
            rows = pl.ds(pl.multiple_of(i * step, step), step)
            stage[slot, 0:wide, rows] = all_ref[rows, start : start + wide].T
            return carry

        lax.fori_loop(0, total // step, body, 0, unroll=True)
        started = []
        for t in range(3):
            lo, hi = max(start, t * WIDTH), min(start + wide, (t + 1) * WIDTH)
            if lo < hi:
                copy = pltpu.make_async_copy(
                    stage.at[slot, lo - start : hi - start],
                    outs[t].at[lo - t * WIDTH : hi - t * WIDTH],
                    sem.at[slot, len(started)],
                )
                copy.start()
                started.append(copy)
        pending[slot] = started
    for started in [lasts, *pending.values()]:
        for copy in started:
            copy.wait()


def local(wg, ag, bg, wu, au, bu, wd, ad, bd, nt, ns):
    rows = 2560
    bf16 = jnp.bfloat16
    hbm = pl.BlockSpec(memory_space=pltpu.HBM)
    inputs = (wg, ag.T, bg, wu, au.T, bu, wd.T, bd, ad.T, nt.reshape(1, -1), ns.reshape(1, -1))
    items = len(CHUNKS) * (SIDE * SIDE - 1)
    vmem = pl.BlockSpec(memory_space=pltpu.VMEM)
    flat_rows = rows // LANE
    gathered = pl.pallas_call(
        gather_kernel,
        out_shape=[
            pltpu.VMEM((rows, COLUMNS), bf16),
            pltpu.VMEM((HALF, rows), bf16),
            pltpu.VMEM((flat_rows, LANE), bf16),
        ],
        in_specs=[hbm] * 11,
        out_specs=[vmem] * 3,
        scratch_shapes=[
            pltpu.VMEM((3, BLOCK, WIDTH), bf16),
            pltpu.VMEM((3, RANK, BLOCK), bf16),
            pltpu.VMEM((3, RANK, WIDTH), bf16),
            pltpu.VMEM((2, 1, nt.shape[0]), jnp.float32),
            pltpu.VMEM((8, 1, LANE), jnp.float32),
            pltpu.VMEM((2 * SIDE * SIDE * FOLD, LANE), bf16),
            pltpu.VMEM((3, 8 * FOLD, 8 * BLOCK), bf16),
            pltpu.VMEM((24, LANE), jnp.float32),
            pltpu.SemaphoreType.DMA((11,)),
            pltpu.SemaphoreType.DMA((items,)),
            pltpu.SemaphoreType.DMA((8,)),
            pltpu.SemaphoreType.DMA((8,)),
            pltpu.SemaphoreType.REGULAR,
            pltpu.SemaphoreType.DMA((2,)),
            pltpu.SemaphoreType.DMA((2,)),
            pltpu.SemaphoreType.DMA((2,)),
        ],
        compiler_params=pltpu.CompilerParams(collective_id=0, has_side_effects=True, vmem_limit_bytes=16 << 20),
        name="gather",
    )(*(pltpu.with_memory_space_constraint(v, pltpu.HBM) for v in inputs))
    gate, up, down, norm = pl.pallas_call(
        turn_kernel,
        out_shape=[jax.ShapeDtypeStruct((WIDTH, rows), bf16)] * 3 + [jax.ShapeDtypeStruct((flat_rows, LANE), bf16)],
        in_specs=[vmem] * 3,
        out_specs=[hbm] * 4,
        scratch_shapes=[
            pltpu.VMEM((4, 256, rows), bf16),
            pltpu.SemaphoreType.DMA((4, 2)),
            pltpu.SemaphoreType.DMA((2,)),
        ],
        compiler_params=pltpu.CompilerParams(vmem_limit_bytes=16 << 20),
        name="turn",
    )(*gathered)
    return gate.T, up.T, down, norm.reshape(rows)


def solution(mesh):
    return jax.shard_map(
        local,
        mesh=mesh,
        in_specs=(
            P("zero", "tp"),
            P("zero", None),
            P(None, "tp"),
            P("zero", "tp"),
            P("zero", None),
            P(None, "tp"),
            P("tp", "zero"),
            P("tp", None),
            P(None, "zero"),
            P(("zero", "tp")),
            P(("zero", "tp")),
        ),
        out_specs=(P(None, "tp"), P(None, "tp"), P("tp", None), P()),
        check_vma=False,
    )
```

```python
import functools
import heapq

import jax
import jax.numpy as jnp
from jax import lax
from jax.experimental import pallas as pl
from jax.experimental.pallas import tpu as pltpu
from jax.sharding import PartitionSpec as P

MESH = pl.DeviceIdType.MESH
LINKS = ("u+", "u-", "v+", "v-")
SIDE = 4
BLOCK = 80
WIDTH = 1216
RANK = 16
LANE = 128
CHUNKS = {"A0": (0, 7), "B1": (21, 28), "A1": (7, 14), "B0": (14, 21), "C0": None}
OWN_US = {"A0": 0.0, "B1": 0.0, "A1": 0.6, "B0": 0.6, "C0": 15.0}
COLUMNS = 28 * LANE
HALF = LANE // 2
FOLD = 48

mix_rate = 0.5


def onward(item):
    chunk, ou, ov = item
    first, second = ("v", "u") if chunk[0] == "B" else ("u", "v")
    a, b = (ov, ou) if chunk[0] == "B" else (ou, ov)
    turn = "+" if chunk[1] == "0" else "-"
    far = SIDE - 1 if turn == "+" else 1
    if b == 0:
        out = [first + "+", first + "-"] if a == 0 else [first + turn] if a == far else []
        return out + [second + "+", second + "-"]
    return [second + turn] if b == far else []


def seen_there(item, link):
    chunk, ou, ov = item
    step = SIDE - 1 if link[1] == "+" else 1
    return (chunk, (ou + step) % SIDE, ov) if link[0] == "u" else (chunk, ou, (ov + step) % SIDE)


def depth(item):
    return max((1 + depth(seen_there(item, link)) for link in onward(item)), default=0)


def plan(tile_us=0.44, hop_us=4.0, leaf_us=3.0):
    free = dict.fromkeys(LINKS, 0.0)
    ready = {link: [] for link in LINKS}
    sends = {link: [] for link in LINKS}
    arrivals, events, count = [], [], 0
    for chunk in CHUNKS:
        events.append((OWN_US[chunk], count, (chunk, 0, 0)))
        count += 1
    while events:
        now, _, item = heapq.heappop(events)
        if item is not None:
            arrivals.append((now + (0.0 if onward(item) else leaf_us), count, item))
            count += 1
            for link in onward(item):
                urgent = depth(seen_there(item, link)) if CHUNKS[item[0]] else 9
                heapq.heappush(ready[link], (-urgent, count, item))
                count += 1
        if events and events[0][0] <= now + 1e-9:
            continue
        for link in LINKS:
            if free[link] <= now + 1e-9 and ready[link]:
                item = heapq.heappop(ready[link])[2]
                lo, hi = CHUNKS[item[0]] or (0, 0.6)
                free[link] = now + (hi - lo) * tile_us
                sends[link].append(item)
                heapq.heappush(events, (free[link], count, None))
                heapq.heappush(events, (free[link] + hop_us, count + 1, seen_there(item, link)))
                count += 2
    return sends, [item for _, _, item in sorted(arrivals)]


def gather_kernel(
    wg, ag, bg, wu, au, bu, wd, ad, bd, nt, ns, all_ref, rest, norm,
    w, a, b, n, nz, folded, picks, flat,
    in_sem, recv_sem, norm_send, norm_recv, ready, send_sem, peer_send, peer_recv,
):
    zero, z = lax.axis_index("zero"), lax.axis_index("tp")
    tp = lax.axis_size("tp")
    core, chip = lax.rem(zero, 2), lax.div(zero, 2)
    x, y = lax.rem(chip, SIDE), lax.div(chip, SIDE)

    def at(ou, ov):
        ox = lax.rem(x + (1 - core) * ou - core * ov + SIDE, SIDE)
        oy = lax.rem(y + (1 - core) * ov - core * ou + SIDE, SIDE)
        return (oy * SIDE + ox) * 2 + core

    place = {(ou, ov): at(ou, ov) for ou in range(SIDE) for ov in range(SIDE)}
    target = {"u+": place[1, 0], "u-": place[3, 0], "v+": place[0, 1], "v-": place[0, 3]}
    peer = zero + 1 - 2 * core

    barrier = pltpu.get_barrier_semaphore()
    for other in list(target.values()) + [peer]:
        pl.semaphore_signal(barrier, inc=1, device_id={"zero": other, "tp": z}, device_id_type=MESH)
    for k in range(1, tp):

        @pl.when(k > z)
        def _():
            pl.semaphore_signal(barrier, inc=1, device_id={"zero": zero, "tp": k}, device_id_type=MESH)

    loads = []
    for k, (src, dst) in enumerate(
        [
            pair
            for t, refs in ((0, (wg, ag, bg)), (2, (wd, ad, bd)), (1, (wu, au, bu)))
            for pair in zip(refs, (w.at[t], a.at[t], b.at[t]))
        ]
        + [(nt, n.at[0]), (ns, n.at[1])]
    ):
        load = pltpu.make_async_copy(src, dst, in_sem.at[k])
        load.start()
        loads.append(load)

    mine = pl.ds(pl.multiple_of(zero * BLOCK, 16), BLOCK)
    cut = WIDTH - HALF

    def latest(t, lo, hi):
        low_high = lax.dot_general(
            a[t], b[t, :, lo:hi], (((0,), (0,)), ((), ())), preferred_element_type=jnp.float32
        )
        return w[t, :, lo:hi].astype(jnp.float32) + mix_rate * low_high

    def keep(first, value):
        all_ref[mine, first : first + value.shape[1]] = value.astype(jnp.bfloat16)

    def arrive(order):
        for load in loads[3 * order : 3 * order + 3]:
            load.wait()

    head = CHUNKS["A0"][1] * LANE
    back = CHUNKS["B1"][0] * LANE - 2 * WIDTH
    arrive(0)
    keep(0, latest(0, 0, head))
    arrive(1)
    keep(2 * WIDTH + back, latest(2, back, cut))

    sends, arrivals = plan()
    number = {item: k for k, item in enumerate(i for i in arrivals if i[1:] != (0, 0))}

    def kind(item):
        return int(CHUNKS[item[0]] is None)

    def span(item):
        chunk, ou, ov = item
        if CHUNKS[chunk] is None:
            return folded.at[pl.ds(pl.multiple_of(place[ou, ov] * FOLD, 16), FOLD)]
        lo, hi = CHUNKS[chunk]
        rows = pl.ds(pl.multiple_of(place[ou, ov] * BLOCK, 16), BLOCK)
        return all_ref.at[rows, lo * LANE : hi * LANE]

    def send(item, link):
        part = span(item)
        pltpu.make_async_remote_copy(
            src_ref=part, dst_ref=part, send_sem=send_sem.at[kind(item)], recv_sem=recv_sem.at[number[seen_there(item, link)]],
            device_id={"zero": target[link], "tp": z}, device_id_type=MESH,
        ).start()

    def hand_over(item):
        part = span(item)
        pltpu.make_async_remote_copy(
            src_ref=part, dst_ref=part, send_sem=peer_send.at[kind(item)], recv_sem=peer_recv.at[kind(item)],
            device_id={"zero": peer, "tp": z}, device_id_type=MESH,
        ).start()

    queue = {link: list(order) for link, order in sends.items()}
    here = set()

    def issue(*items):
        here.update(items)
        moved = True
        while moved:
            moved = False
            for link in LINKS:
                if queue[link] and queue[link][0] in here:
                    send(queue[link].pop(0), link)
                    moved = True
        for item in items:
            hand_over(item)

    def norm_copy(k):
        return pltpu.make_async_remote_copy(
            src_ref=nz.at[z], dst_ref=nz.at[z], send_sem=norm_send.at[k], recv_sem=norm_recv.at[z],
            device_id={"zero": zero, "tp": k}, device_id_type=MESH,
        )

    pl.semaphore_wait(barrier, len(target) + 1 + z)
    issue(("A0", 0, 0), ("B1", 0, 0))

    keep(2 * WIDTH, latest(2, 0, back))
    arrive(2)
    keep(head, jnp.concatenate([latest(0, head, WIDTH), latest(1, 0, WIDTH)], axis=1))
    loads[9].wait()
    loads[10].wait()
    gain = (n[0] + n[1]).astype(jnp.bfloat16).astype(jnp.float32)
    nz[z] = jnp.concatenate([gain, jnp.zeros((1, LANE - gain.shape[1]), jnp.float32)], axis=1)
    issue(("A1", 0, 0), ("B0", 0, 0))

    for k in range(tp - 1):

        @pl.when(k < z)
        def _():
            pl.semaphore_signal(ready, inc=1, device_id={"zero": zero, "tp": k}, device_id_type=MESH)
            norm_copy(k).start()

    wide = 8 * BLOCK

    def make_picks():
        for e in range(8):
            r = lax.broadcasted_iota(jnp.int32, (FOLD, wide), 0)
            c = lax.broadcasted_iota(jnp.int32, (FOLD, wide), 1) - e * BLOCK
            half = BLOCK // 2
            for m, hit in enumerate(
                [(c == r) & (r < half), (c == r + half) & (r < half), (r == half) & (c >= 0) & (c < BLOCK)]
            ):
                picks[m, e * FOLD : (e + 1) * FOLD] = jnp.where(hit, 1.0, 0.0).astype(jnp.bfloat16)

    def unfold(g):
        rows = folded[g * 8 * FOLD : (g + 1) * 8 * FOLD]
        left, right, line = (
            lax.dot_general(rows, picks[m], (((0,), (0,)), ((), ())), preferred_element_type=jnp.float32)
            for m in range(3)
        )
        rest[:, g * wide : (g + 1) * wide] = (left[:HALF] + right[HALF:]).astype(jnp.bfloat16)
        i = lax.broadcasted_iota(jnp.int32, (BLOCK, wide), 0)
        l = lax.broadcasted_iota(jnp.int32, (BLOCK, wide), 1)
        own = functools.reduce(jnp.logical_or, [i + e * BLOCK == l for e in range(8)])
        gains = jnp.sum(jnp.where(own, line[:BLOCK], 0.0), axis=0, keepdims=True)
        for k in range(wide // LANE):
            at_row = g * (wide // LANE) + k
            flat[at_row : at_row + 1] = gains[:, k * LANE : (k + 1) * LANE]

    c_left = sum(kind(item) for item in arrivals) - 1
    groups = list(range(all_ref.shape[0] // wide))
    waited, stored = 0, []
    for item in arrivals:
        if item == ("C0", 0, 0):
            for k in range(tp):

                @pl.when(k != z)
                def _():
                    pltpu.make_async_remote_copy(
                        src_ref=nz.at[k], dst_ref=nz.at[k], send_sem=norm_send.at[k], recv_sem=norm_recv.at[k],
                        device_id={"zero": zero, "tp": k}, device_id_type=MESH,
                    ).wait_recv()

            share = BLOCK // tp
            gains = [nz[k][:, :share] for k in range(tp)] + [jnp.zeros((1, LANE - BLOCK), jnp.float32)]
            gains = jnp.concatenate(gains, axis=1)
            left = latest(2, cut, WIDTH)
            top = jnp.concatenate([left[: BLOCK // 2], left[BLOCK // 2 :]], axis=1)
            line = lax.broadcasted_iota(jnp.int32, (FOLD - BLOCK // 2, LANE), 0)
            bottom = jnp.where(line == 0, jnp.broadcast_to(gains, line.shape), 0.0)
            fold = jnp.concatenate([top, bottom], axis=0).astype(jnp.bfloat16)
            folded[pl.ds(pl.multiple_of(zero * FOLD, 16), FOLD)] = fold
            stored.append(item)
        elif item[1:] != (0, 0):
            part = span(item)
            pltpu.make_async_remote_copy(
                src_ref=part, dst_ref=part, send_sem=send_sem.at[kind(item)], recv_sem=recv_sem.at[number[item]],
                device_id={"zero": peer, "tp": z}, device_id_type=MESH,
            ).wait_recv()
            issue(item, *stored)
            stored.clear()
            waited += 1
            c_left -= kind(item)
            if waited == 6:
                make_picks()
            if c_left == 0 and kind(item):
                folds = folded.at[0 : SIDE * SIDE * FOLD]
                pltpu.make_async_copy(folds, folds, peer_recv.at[1]).wait()
            elif c_left == 0 and groups:
                unfold(groups.pop(0))
            if waited == 8:

                @pl.when(z < tp - 1)
                def _():
                    pl.semaphore_wait(ready, tp - 1 - z)

                for k in range(1, tp):

                    @pl.when(k > z)
                    def _():
                        norm_copy(k).start()

    assert not any(queue.values()) and not groups

    norm[...] = flat[0 : norm.shape[0]].astype(jnp.bfloat16)
    blocks = SIDE * SIDE
    for sem, count, buffer, rows in (
        (peer_recv.at[0], blocks, all_ref, BLOCK),
        (peer_send.at[0], blocks, all_ref, BLOCK),
        (peer_send.at[1], blocks, folded, FOLD),
        (send_sem.at[0], blocks - 1, all_ref, BLOCK),
        (send_sem.at[1], blocks - 1, folded, FOLD),
    ):
        whole = buffer.at[0 : count * rows]
        pltpu.make_async_copy(whole, whole, sem).wait()
    for k in range(tp):

        @pl.when(k != z)
        def _():
            norm_copy(k).wait_send()


def turn_kernel(all_ref, rest, norm_rows, gate, up, down, norm, stage, sem, rest_sem):
    outs = (gate, up, down)
    total = all_ref.shape[0]
    size, step = stage.shape[1], LANE
    lasts = [
        pltpu.make_async_copy(rest, down.at[WIDTH - HALF : WIDTH], rest_sem.at[0]),
        pltpu.make_async_copy(norm_rows, norm, rest_sem.at[1]),
    ]
    for copy in lasts:
        copy.start()
    pending = {}
    half = size // 2
    blocks = [(0, half), (half, half)] + [(start, size) for start in range(size, COLUMNS, size)]
    for order, (start, wide) in enumerate(blocks):
        slot = order % stage.shape[0]
        for copy in pending.pop(slot, ()):
            copy.wait()

        def body(i, carry):
            rows = pl.ds(pl.multiple_of(i * step, step), step)
            stage[slot, 0:wide, rows] = all_ref[rows, start : start + wide].T
            return carry

        lax.fori_loop(0, total // step, body, 0, unroll=True)
        started = []
        for t in range(3):
            lo, hi = max(start, t * WIDTH), min(start + wide, (t + 1) * WIDTH)
            if lo < hi:
                copy = pltpu.make_async_copy(
                    stage.at[slot, lo - start : hi - start],
                    outs[t].at[lo - t * WIDTH : hi - t * WIDTH],
                    sem.at[slot, len(started)],
                )
                copy.start()
                started.append(copy)
        pending[slot] = started
    for started in [lasts, *pending.values()]:
        for copy in started:
            copy.wait()


def local(wg, ag, bg, wu, au, bu, wd, ad, bd, nt, ns):
    rows = 2560
    bf16 = jnp.bfloat16
    hbm = pl.BlockSpec(memory_space=pltpu.HBM)
    inputs = (wg, ag.T, bg, wu, au.T, bu, wd.T, bd, ad.T, nt.reshape(1, -1), ns.reshape(1, -1))
    items = len(CHUNKS) * (SIDE * SIDE - 1)
    vmem = pl.BlockSpec(memory_space=pltpu.VMEM)
    flat_rows = rows // LANE
    gathered = pl.pallas_call(
        gather_kernel,
        out_shape=[
            pltpu.VMEM((rows, COLUMNS), bf16),
            pltpu.VMEM((HALF, rows), bf16),
            pltpu.VMEM((flat_rows, LANE), bf16),
        ],
        in_specs=[hbm] * 11,
        out_specs=[vmem] * 3,
        scratch_shapes=[
            pltpu.VMEM((3, BLOCK, WIDTH), bf16),
            pltpu.VMEM((3, RANK, BLOCK), bf16),
            pltpu.VMEM((3, RANK, WIDTH), bf16),
            pltpu.VMEM((2, 1, nt.shape[0]), jnp.float32),
            pltpu.VMEM((8, 1, LANE), jnp.float32),
            pltpu.VMEM((2 * SIDE * SIDE * FOLD, LANE), bf16),
            pltpu.VMEM((3, 8 * FOLD, 8 * BLOCK), bf16),
            pltpu.VMEM((24, LANE), jnp.float32),
            pltpu.SemaphoreType.DMA((11,)),
            pltpu.SemaphoreType.DMA((items,)),
            pltpu.SemaphoreType.DMA((8,)),
            pltpu.SemaphoreType.DMA((8,)),
            pltpu.SemaphoreType.REGULAR,
            pltpu.SemaphoreType.DMA((2,)),
            pltpu.SemaphoreType.DMA((2,)),
            pltpu.SemaphoreType.DMA((2,)),
        ],
        compiler_params=pltpu.CompilerParams(collective_id=0, has_side_effects=True, vmem_limit_bytes=16 << 20),
        name="gather",
    )(*(pltpu.with_memory_space_constraint(v, pltpu.HBM) for v in inputs))
    gate, up, down, norm = pl.pallas_call(
        turn_kernel,
        out_shape=[jax.ShapeDtypeStruct((WIDTH, rows), bf16)] * 3 + [jax.ShapeDtypeStruct((flat_rows, LANE), bf16)],
        in_specs=[vmem] * 3,
        out_specs=[hbm] * 4,
        scratch_shapes=[
            pltpu.VMEM((4, 256, rows), bf16),
            pltpu.SemaphoreType.DMA((4, 2)),
            pltpu.SemaphoreType.DMA((2,)),
        ],
        compiler_params=pltpu.CompilerParams(vmem_limit_bytes=16 << 20),
        name="turn",
    )(*gathered)
    return gate.T, up.T, down, norm.reshape(rows)


def solution(mesh):
    return jax.shard_map(
        local,
        mesh=mesh,
        in_specs=(
            P("zero", "tp"),
            P("zero", None),
            P(None, "tp"),
            P("zero", "tp"),
            P("zero", None),
            P(None, "tp"),
            P("tp", "zero"),
            P("tp", None),
            P(None, "zero"),
            P(("zero", "tp")),
            P(("zero", "tp")),
        ),
        out_specs=(P(None, "tp"), P(None, "tp"), P("tp", None), P()),
        check_vma=False,
    )
```
